32 devices in a mesh: dp: 4 (over z), tp: 8 (over y, x, core).
Axes of the slice: x: 2, y: 2, z: 4, core: 2. Of those that a mesh axis runs over, the one named last changes fastest.
Arguments:
- hidden: bfloat16 [8192, 576], P('dp')
- w_final: float32 [576], replicated
- emb_table: bfloat16 [49152, 576], P('tp')
- teacher: bfloat16 [8192, 49152], P('dp', 'tp')
- tok_mask: float32 [8192], P('dp')
Outputs:
- output 1: float32 [], replicated
- output 2: bfloat16 [8192, 576], P('dp')
- output 3: float32 [576], replicated
- output 4: float32 [49152, 576], P('tp')
All inputs are finite; a program needn't handle non-finite values.
Results may differ from the reference program's by a relative error of at most 0.00101509.
Values sent between devices are 32-bit elements.
A program may use at most 1 GiB of HBM per device.

```python
import math
import jax
import jax.numpy as jnp
from jax import lax

MODEL_DIM = 576
VOCAB_SIZE = 49152
NUM_TOKENS = 8192
SEQ_LEN = 16
ROW_BLOCK = math.gcd(NUM_TOKENS, 64)
SOFT_CAP = 30.0
NORM_EPS = 1e-6


def setup_inputs(seed: int = 0) -> dict:
    root_key = jax.random.key(seed)
    k_hid, k_gain, k_dir, k_tab, k_off, k_tea, k_seq, k_tok = jax.random.split(root_key, 8)
    fan_scale = 1.0 / math.sqrt(MODEL_DIM)
    hidden = 3.0 * jax.random.normal(k_hid, (NUM_TOKENS, MODEL_DIM), jnp.float32)
    w_final = 0.3 * jax.random.normal(k_gain, (MODEL_DIM,), jnp.float32)
    direction = 15.0 * fan_scale * jax.random.normal(k_dir, (MODEL_DIM,), jnp.float32)
    emb_table = direction[None, :] + 2.0 * fan_scale * jax.random.normal(k_tab, (VOCAB_SIZE, MODEL_DIM), jnp.float32)
    offset = 15.0 * jax.random.normal(k_off, (NUM_TOKENS, 1), jnp.float32)
    teacher = offset + 3.0 * jax.random.normal(k_tea, (NUM_TOKENS, VOCAB_SIZE), jnp.float32)
    seq_keep = (jax.random.randint(k_seq, (NUM_TOKENS // SEQ_LEN,), 0, 4) > 0).at[0].set(True)
    tok_keep = (jax.random.randint(k_tok, (NUM_TOKENS,), 0, 8) > 0).at[0].set(True)
    tok_mask = jnp.logical_and(jnp.repeat(seq_keep, SEQ_LEN), tok_keep).astype(jnp.float32)
    return {'hidden': hidden.astype(jnp.bfloat16), 'w_final': w_final, 'emb_table': emb_table.astype(jnp.bfloat16), 'teacher': teacher.astype(jnp.bfloat16), 'tok_mask': tok_mask}


def final_norm(hid_rows, w_final):
    hid_f = hid_rows.astype(jnp.float32)
    inv_rms = lax.rsqrt(jnp.mean(hid_f * hid_f, axis=-1, keepdims=True) + NORM_EPS)
    normed = hid_f * inv_rms
    return inv_rms, normed, (normed * (1.0 + w_final)).astype(jnp.bfloat16)


def reference(hidden, w_final, emb_table, teacher, tok_mask):
    mask_sum = jnp.sum(tok_mask)
    num_blocks = NUM_TOKENS // ROW_BLOCK
    hid_blocks = hidden.reshape(num_blocks, ROW_BLOCK, MODEL_DIM)
    tea_blocks = teacher.reshape(num_blocks, ROW_BLOCK, VOCAB_SIZE)
    mask_blocks = tok_mask.reshape(num_blocks, ROW_BLOCK)

    def block_step(scan_carry, block_in):
        loss_acc, gain_acc, table_acc = scan_carry
        hid_rows, tea_rows, mask_rows = block_in
        inv_rms, normed, x_rows = final_norm(hid_rows, w_final)
        logits = jnp.dot(x_rows, emb_table.T, preferred_element_type=jnp.float32)
        stu_cap = SOFT_CAP * jnp.tanh(logits / SOFT_CAP)
        tea_cap = SOFT_CAP * jnp.tanh(tea_rows.astype(jnp.float32) / SOFT_CAP)
        stu_logp = stu_cap - jax.nn.logsumexp(stu_cap, axis=-1, keepdims=True)
        tea_logp = tea_cap - jax.nn.logsumexp(tea_cap, axis=-1, keepdims=True)
        tea_prob = jnp.exp(tea_logp)
        kl_rows = jnp.sum(tea_prob * (tea_logp - stu_logp), axis=-1)
        weight = (mask_rows / mask_sum)[:, None]
        cap_ratio = stu_cap / SOFT_CAP
        grad_z = ((jnp.exp(stu_logp) - tea_prob) * weight * (1.0 - cap_ratio * cap_ratio)).astype(jnp.bfloat16)
        grad_x = jnp.dot(grad_z, emb_table, preferred_element_type=jnp.float32)
        grad_n = grad_x * (1.0 + w_final)
        grad_h = inv_rms * (grad_n - normed * jnp.mean(grad_n * normed, axis=-1, keepdims=True))
        loss_acc = loss_acc + jnp.sum(mask_rows * kl_rows)
        gain_acc = gain_acc + jnp.sum(grad_x * normed, axis=0)
        table_acc = table_acc + jnp.dot(grad_z.T, x_rows, preferred_element_type=jnp.float32)
        return (loss_acc, gain_acc, table_acc), grad_h.astype(jnp.bfloat16)

    init_carry = (jnp.zeros((), jnp.float32), jnp.zeros((MODEL_DIM,), jnp.float32), jnp.zeros((VOCAB_SIZE, MODEL_DIM), jnp.float32))
    (loss_acc, gain_acc, table_acc), grad_blocks = lax.scan(block_step, init_carry, (hid_blocks, tea_blocks, mask_blocks))
    return loss_acc / mask_sum, grad_blocks.reshape(NUM_TOKENS, MODEL_DIM), gain_acc, table_acc
```

```python
import functools
import jax, jax.numpy as jnp
from jax import lax
from jax.experimental import pallas as pl
from jax.experimental.pallas import tpu as pltpu

from jax.sharding import PartitionSpec as P

MESH = pl.DeviceIdType.MESH
SOFT_CAP = 30.0
CAP_INV = 1.0 / 30.0
CAP_LOG2E = 30.0 * 1.4426950408889634
NORM_EPS = 1e-6
D = 576

def stats_kernel(vt, rs, hid_ref, w_ref, tab_ref, tea_ref, x_ref, xt_ref, st_ref, acc):
    hid = hid_ref[...].astype(jnp.float32)
    inv = lax.rsqrt(jnp.sum(hid * hid, axis=0, keepdims=True) * (1.0 / D) + NORM_EPS)
    xt = hid * inv * (1.0 + w_ref[...])
    xt_ref[...] = xt.astype(jnp.bfloat16)
    x_ref[...] = jnp.transpose(xt).astype(jnp.bfloat16)
    acc[...] = jnp.zeros_like(acc)
    nv = tab_ref.shape[1] // vt
    tb = x_ref.shape[0]

    def step(j, carry):
        cols = pl.ds(pl.multiple_of(j * vt, vt), vt)
        tab = tab_ref[:, cols]
        for i in range(tb // rs):
            rows = pl.ds(i * rs, rs)
            z = jnp.dot(x_ref[rows, :], tab, preferred_element_type=jnp.float32)
            ths = jnp.tanh(z * CAP_INV)
            es = jnp.exp2(ths * CAP_LOG2E)
            tht = jnp.tanh(tea_ref[rows, cols].astype(jnp.float32) * CAP_INV)
            et = jnp.exp2(tht * CAP_LOG2E)
            wt = et * (tht - ths)
            def fold(a):
                r = a[:, 0:128]
                for k in range(1, vt // 128):
                    r = r + a[:, k * 128:(k + 1) * 128]
                return r
            acc[0, rows, :] += fold(es)
            acc[1, rows, :] += fold(et)
            acc[2, rows, :] += fold(wt)
        return carry
    lax.fori_loop(0, nv, step, 0)
    for k in range(3):
        sums = jnp.sum(jnp.transpose(acc[k]), axis=0, keepdims=True)
        for q in range(tb // 128):
            st_ref[pl.ds((k * pl.num_programs(0) + pl.program_id(0)) * (tb // 128) + q, 1), :] = sums[:, q * 128:(q + 1) * 128]


def forward(hid_t, w_col, tab_t, tea, tb=256, vt=2048, rs=128):
    t, v = tea.shape
    return pl.pallas_call(
        functools.partial(stats_kernel, vt, rs),
        grid=(t // tb,),
        out_shape=(jax.ShapeDtypeStruct((t, D), jnp.bfloat16), jax.ShapeDtypeStruct((D, t), jnp.bfloat16), jax.ShapeDtypeStruct((3 * t // 128, 128), jnp.float32)),
        in_specs=[pl.BlockSpec((D, tb), lambda i: (0, i)), pl.BlockSpec((D, 1), lambda i: (0, 0)), pl.BlockSpec((D, v), lambda i: (0, 0), pipeline_mode=pl.Buffered(1)), pl.BlockSpec((tb, v), lambda i: (i, 0))],
        out_specs=(pl.BlockSpec((tb, D), lambda i: (i, 0)), pl.BlockSpec((D, tb), lambda i: (0, i)), pl.BlockSpec((3 * t // 128, 128), lambda i: (0, 0))),
        scratch_shapes=[pltpu.VMEM((3, tb, 128), jnp.float32)],
        compiler_params=pltpu.CompilerParams(vmem_limit_bytes=48 * 1024 * 1024),
        name='forward',
    )(hid_t, w_col, tab_t, tea)


VBLK = 256
TBLK = 256
NPART = 3
PROWS = D // NPART


def backward_kernel(nblk, ntok, tp, dp, x_ref, xt_ref, st_ref, mask_ref, w_ref, hid_ref, tab_ref, tea_ref,
                    out_ref, dh_ref, small_ref, land_ref, gath_ref,
                    part, near, far, dxt, gbuf, tea_buf, tab_buf, coef_s, coef_t, sbuf, mbuf, slab, load, stage, hbuf, acc_a, acc_b, mloc,
                    blk_sem, send1, recv1, send2, recv2, send3, recv3, store_sem, ssem, srecv, msem, mrecv, rsem, rrecv, gsem, grecv,
                    asem, arecv, bsem, brecv, lsem, hsem, osem):
    z = lax.axis_index('dp')
    t = lax.axis_index('tp')
    inner = jnp.logical_or(z == 1, z == 2)
    outer = jnp.logical_or(z == 0, z == 3)
    across = 3 - z
    beside = jnp.where(z < 2, 1 - z, 5 - z)
    nch = nblk * NPART
    ntile = ntok // TBLK
    rows16 = ntok // 128
    slice_cols = ntok // tp

    def remote(src, dst, ssem_, rsem_, **where):
        return pltpu.make_async_remote_copy(src_ref=src, dst_ref=dst, send_sem=ssem_, recv_sem=rsem_, device_id=where, device_id_type=MESH)

    def tea_load(b):
        return pltpu.make_async_copy(tea_ref.at[:, pl.ds(pl.multiple_of(b * VBLK, VBLK), VBLK)], tea_buf.at[b % 2], blk_sem.at[0, b % 2])

    def tab_load(b):
        return pltpu.make_async_copy(tab_ref.at[:, pl.ds(pl.multiple_of(b * VBLK, VBLK), VBLK)], tab_buf.at[b % 2], blk_sem.at[1, b % 2])

    tea_load(0).start()
    tab_load(0).start()
    hid_load = pltpu.make_async_copy(hid_ref.at[:, pl.ds(pl.multiple_of(t * slice_cols, slice_cols), slice_cols)], hbuf, hsem)
    hid_load.start()
    mloc[...] = mask_ref[0:8, :] + mask_ref[8:16, :]

    barrier = pltpu.get_barrier_semaphore()
    for i in range(1, tp):
        pl.semaphore_signal(barrier, inc=1, device_id={'tp': lax.rem(t + i, tp)}, device_id_type=MESH)
    for i in range(1, dp):
        pl.semaphore_signal(barrier, inc=1, device_id={'dp': lax.rem(z + i, dp)}, device_id_type=MESH)
    pl.semaphore_wait(barrier, tp + dp - 2)

    for i in range(1, tp):
        remote(st_ref, sbuf.at[t], ssem.at[i], srecv.at[t], tp=lax.rem(t + i, tp)).start()
    for i in range(1, dp):
        remote(mloc, mbuf.at[z], msem.at[i], mrecv.at[z], dp=lax.rem(z + i, dp)).start()
    sbuf[t] = st_ref[...]
    mbuf[z] = mloc[...]
    for i in range(1, tp):
        j = lax.rem(t + i, tp)
        remote(st_ref, sbuf.at[j], ssem.at[i], srecv.at[j], tp=j).wait_recv()
    for i in range(1, dp):
        j = lax.rem(z + i, dp)
        remote(mloc, mbuf.at[j], msem.at[i], mrecv.at[j], dp=j).wait_recv()
    sums = sbuf[0]
    for i in range(1, tp):
        sums = sums + sbuf[i]
    count = mbuf[0]
    for i in range(1, dp):
        count = count + mbuf[i]
    mask_sum = jnp.sum(jnp.sum(count, axis=0, keepdims=True), axis=1, keepdims=True)
    stu_sum, tea_sum, cross = sums[0:rows16], sums[rows16:2 * rows16], sums[2 * rows16:3 * rows16]
    mask = mask_ref[...]
    kl = SOFT_CAP * cross / tea_sum + jnp.log(stu_sum) - jnp.log(tea_sum)
    lrow = jnp.sum(mask * kl, axis=0, keepdims=True)
    weight = mask / mask_sum
    for coef, norm in ((coef_s, stu_sum), (coef_t, tea_sum)):
        ratio = weight / norm
        for r in range(rows16):
            coef[r * 128:(r + 1) * 128, :] = jnp.transpose(jnp.broadcast_to(ratio[r:r + 1, :], (128, 128)))
    dxt[...] = jnp.zeros_like(dxt)

    def compute(b):
        slot = b % 2
        tea_load(b).wait()
        tab_load(b).wait()

        @pl.when(b + 1 < nblk)
        def _():
            tea_load(b + 1).start()
            tab_load(b + 1).start()

        def tile(i, carry):
            rows = pl.ds(pl.multiple_of(i * TBLK, TBLK), TBLK)
            tab = tab_buf[slot]
            logits = jnp.dot(x_ref[rows, :], tab, preferred_element_type=jnp.float32)
            ths = jnp.tanh(logits * CAP_INV)
            tht = jnp.tanh(tea_buf[slot, rows, :].astype(jnp.float32) * CAP_INV)
            cs, ct = coef_s[rows, :], coef_t[rows, :]
            cs2 = jnp.concatenate([cs, cs], axis=1)
            ct2 = jnp.concatenate([ct, ct], axis=1)
            g = (jnp.exp2(ths * CAP_LOG2E) * cs2 - jnp.exp2(tht * CAP_LOG2E) * ct2) * (1.0 - ths * ths)
            g = g.astype(jnp.bfloat16)
            gbuf[rows, :] = g
            dxt[:, rows] += lax.dot_general(tab, g, (((1,), (1,)), ((), ())), preferred_element_type=jnp.float32)
            return carry
        lax.fori_loop(0, ntile, tile, 0)
        part[pl.ds(b * NPART, NPART)] = jnp.dot(xt_ref[...], gbuf[...], preferred_element_type=jnp.float32).reshape(NPART, PROWS, VBLK)

        @pl.when(outer)
        def _():
            for q in range(NPART):
                c = b * NPART + q
                remote(part.at[c], near.at[c], send1, recv1.at[c], dp=beside).start()

    def place(c):
        return out_ref.at[pl.ds(pl.multiple_of((c % NPART) * PROWS, PROWS), PROWS), pl.ds(pl.multiple_of((c // NPART) * VBLK, VBLK), VBLK)]

    def swap(c):
        return remote(part.at[c], far.at[c], send2, recv2.at[c], dp=across)

    def first(c):
        remote(part.at[c], near.at[c], send1, recv1.at[c], dp=beside).wait_recv()
        part[c] = part[c] + near[c]
        swap(c).start()

    def finish(c):
        swap(c).wait_recv()
        far[c] = far[c] + part[c]
        remote(far.at[c], place(c), send3, recv3, dp=beside).start()
        pltpu.make_async_copy(far.at[c], place(c), store_sem).start()

    def comm(k):
        @pl.when(inner)
        def _():
            first(k)

            @pl.when(k > 0)
            def _():
                finish(k - 1)

    def loop(lo, hi, body):
        def step(k, carry):
            body(k)
            return carry
        lax.fori_loop(lo, hi, step, 0)

    compute(0)

    def both(k):
        compute(k + 1)
        comm(k)
    loop(0, nblk - 1, both)

    def cols_of(j):
        return pl.ds(pl.multiple_of(j * slice_cols, slice_cols), slice_cols)
    for i in range(1, tp):
        j = lax.rem(t + i, tp)
        remote(dxt.at[:, cols_of(j)], land_ref.at[t], rsem.at[i], rrecv.at[t], tp=j).start()
    k1 = nblk - 1
    k2 = k1 + 14
    loop(k1, k2, comm)
    stage[...] = dxt[:, cols_of(t)]

    def gather(k):
        i = k - k2 + 1
        j = lax.rem(t + i, tp)
        remote(dxt.at[:, cols_of(j)], land_ref.at[j], rsem.at[i], rrecv.at[j], tp=j).wait_recv()
        copy = pltpu.make_async_copy(land_ref.at[j], load, lsem)
        copy.start()
        comm(k)
        copy.wait()
        stage[...] += load[...]
    loop(k2, k2 + tp - 1, gather)
    k3 = k2 + tp - 1
    hid_load.wait()
    hid = hbuf[...].astype(jnp.float32)
    inv = lax.rsqrt(jnp.sum(hid * hid, axis=0, keepdims=True) * (1.0 / D) + NORM_EPS)
    normed = hid * inv
    dx = stage[...]
    gain = dx * normed
    gain = sum((gain[:, q * 128:(q + 1) * 128] for q in range(1, slice_cols // 128)), gain[:, 0:128])
    load[...] = jnp.zeros_like(load)
    load[0:D, 0:128] = gain
    slab[...] = jnp.zeros_like(slab)
    for q in range(5):
        lo, hi = q * 128, min(D, q * 128 + 128)
        sq = load[lo:hi, 0:128]
        if hi - lo < 128:
            sq = jnp.concatenate([sq, jnp.zeros((128 - (hi - lo), 128), jnp.float32)], axis=0)
        slab[0:1, lo:lo + 128] = jnp.sum(jnp.transpose(sq), axis=0, keepdims=True)
    slab[1:2, 0:128] = lrow
    grad_n = dx * (1.0 + w_ref[...])
    stage[...] = inv * (grad_n - normed * (jnp.sum(grad_n * normed, axis=0, keepdims=True) * (1.0 / D)))
    for i in range(1, tp):
        j = lax.rem(t + i, tp)
        remote(slab, acc_a.at[t], asem.at[i], arecv.at[t], tp=j).start()
        remote(stage, gath_ref.at[t], gsem.at[i], grecv.at[t], tp=j).start()
    acc_a[t] = slab[...]

    def emit(j):
        hbuf[...] = load[...].astype(jnp.bfloat16)
        copy = pltpu.make_async_copy(hbuf, dh_ref.at[:, cols_of(j)], hsem)
        copy.start()
        copy.wait()
    load[...] = stage[...]
    emit(t)
    k4 = k3 + 14
    loop(k3, k4, comm)
    for i in range(1, tp):
        j = lax.rem(t + i, tp)
        remote(slab, acc_a.at[j], asem.at[i], arecv.at[j], tp=j).wait_recv()
    tot = acc_a[0]
    for i in range(1, tp):
        tot = tot + acc_a[i]
    hbuf_row = lax.broadcasted_iota(jnp.int32, tot.shape, 0) == 0
    acc_b[z] = jnp.where(hbuf_row, tot, slab[...])
    for i in range(1, dp):
        j = lax.rem(z + i, dp)
        remote(acc_b.at[z], acc_b.at[z], bsem.at[i], brecv.at[z], dp=j).start()

    def spread(k):
        i = k - k4 + 1
        j = lax.rem(t + i, tp)
        remote(stage, gath_ref.at[j], gsem.at[i], grecv.at[j], tp=j).wait_recv()
        copy = pltpu.make_async_copy(gath_ref.at[j], load, lsem)
        copy.start()
        comm(k)
        copy.wait()
        emit(j)
    loop(k4, k4 + tp - 1, spread)
    loop(k4 + tp - 1, nch, comm)

    for i in range(1, dp):
        j = lax.rem(z + i, dp)
        remote(acc_b.at[j], acc_b.at[j], bsem.at[i], brecv.at[j], dp=j).wait_recv()
    tot = acc_b[0]
    for i in range(1, dp):
        tot = tot + acc_b[i]
    loss = jnp.sum(tot[1:2, 0:128], axis=1, keepdims=True) / mask_sum
    row = lax.broadcasted_iota(jnp.int32, tot.shape, 0)
    small_ref[...] = jnp.where(row == 1, loss, tot)

    @pl.when(inner)
    def _():
        finish(nch - 1)
        remote(part, far, send2, recv2.at[0], dp=across).wait_send()
        remote(far, far, send3, recv3, dp=beside).wait_send()
        pltpu.make_async_copy(out_ref, out_ref, store_sem).wait()

    @pl.when(outer)
    def _():
        remote(part, near, send1, recv1.at[0], dp=beside).wait_send()
        remote(out_ref, out_ref, send3, recv3, dp=beside).wait_recv()

    for i in range(1, tp):
        j = lax.rem(t + i, tp)
        remote(st_ref, sbuf.at[t], ssem.at[i], srecv.at[t], tp=j).wait_send()
        remote(dxt.at[:, cols_of(j)], land_ref.at[t], rsem.at[i], rrecv.at[t], tp=j).wait_send()
        remote(slab, acc_a.at[t], asem.at[i], arecv.at[t], tp=j).wait_send()
        remote(stage, gath_ref.at[t], gsem.at[i], grecv.at[t], tp=j).wait_send()
    for i in range(1, dp):
        j = lax.rem(z + i, dp)
        remote(mloc, mbuf.at[z], msem.at[i], mrecv.at[z], dp=j).wait_send()
        remote(acc_b.at[z], acc_b.at[z], bsem.at[i], brecv.at[z], dp=j).wait_send()


def backward(mesh, x, xt, stats, mask, w_col, hid_t, tab_t, tea):
    tp, dp = mesh.shape['tp'], mesh.shape['dp']
    ntok, vocab = tea.shape
    nblk = vocab // VBLK
    nch = nblk * NPART
    sl = ntok // tp
    f32, bf16 = jnp.float32, jnp.bfloat16
    dma = pltpu.SemaphoreType.DMA
    vmem = pl.BlockSpec(memory_space=pltpu.VMEM)
    hbm = pl.BlockSpec(memory_space=pl.ANY)
    chunks = pltpu.VMEM((nch, PROWS, VBLK), f32)
    out, dh, small, _, _ = pl.pallas_call(
        functools.partial(backward_kernel, nblk, ntok, tp, dp),
        out_shape=(jax.ShapeDtypeStruct((D, vocab), f32), jax.ShapeDtypeStruct((D, ntok), bf16), jax.ShapeDtypeStruct((8, 640), f32),
                   jax.ShapeDtypeStruct((tp, D, sl), f32), jax.ShapeDtypeStruct((tp, D, sl), f32)),
        in_specs=[vmem, vmem, vmem, vmem, vmem, hbm, hbm, hbm],
        out_specs=(hbm, hbm, vmem, hbm, hbm),
        scratch_shapes=[
            chunks, chunks, chunks, pltpu.VMEM((D, ntok), f32), pltpu.VMEM((ntok, VBLK), bf16), pltpu.VMEM((2, ntok, VBLK), bf16),
            pltpu.VMEM((2, D, VBLK), bf16), pltpu.VMEM((ntok, 128), f32), pltpu.VMEM((ntok, 128), f32), pltpu.VMEM((tp, 3 * ntok // 128, 128), f32),
            pltpu.VMEM((dp, 8, 128), f32), pltpu.VMEM((8, 640), f32), pltpu.VMEM((D, sl), f32), pltpu.VMEM((D, sl), f32), pltpu.VMEM((D, sl), bf16),
            pltpu.VMEM((tp, 8, 640), f32), pltpu.VMEM((dp, 8, 640), f32), pltpu.VMEM((8, 128), f32),
            dma((2, 2)), dma, dma((nch,)), dma, dma((nch,)), dma, dma, dma, dma((tp,)), dma((tp,)), dma((dp,)), dma((dp,)),
            dma((tp,)), dma((tp,)), dma((tp,)), dma((tp,)), dma((tp,)), dma((tp,)), dma((dp,)), dma((dp,)), dma, dma, dma],
        compiler_params=pltpu.CompilerParams(collective_id=0, has_side_effects=True, vmem_limit_bytes=67043328),
        name='backward',
    )(x, xt, stats, mask, w_col, hid_t, tab_t, tea)
    return out, dh, small


def solution(mesh):
    def local_step(hid_rows, w_final, tab_rows, tea_rows, mask_rows):
        w_col = w_final[:, None]
        hid_t, tab_t = hid_rows.T, tab_rows.T
        x, xt, stats = forward(hid_t, w_col, tab_t, tea_rows)
        mask = mask_rows.reshape(-1, 128)
        grad_table, grad_hid, small = backward(mesh, x, xt, stats, mask, w_col, hid_t, tab_t, tea_rows)
        return small[1, 0], grad_hid.T, small[0, :D], grad_table.T

    return jax.shard_map(local_step, mesh=mesh, in_specs=(P('dp', None), P(None), P('tp', None), P('dp', 'tp'), P('dp')), out_specs=(P(), P('dp', None), P(None), P('tp', None)), check_vma=False)
```

```python
import functools
import jax, jax.numpy as jnp
from jax import lax
from jax.experimental import pallas as pl
from jax.experimental.pallas import tpu as pltpu

from jax.sharding import PartitionSpec as P

MESH = pl.DeviceIdType.MESH
SOFT_CAP = 30.0
CAP_INV = 1.0 / 30.0
CAP_LOG2E = 30.0 * 1.4426950408889634
NORM_EPS = 1e-6
D = 576

def stats_kernel(vt, rs, hid_ref, w_ref, tab_ref, tea_ref, x_ref, xt_ref, st_ref, acc):
    hid = hid_ref[...].astype(jnp.float32)
    inv = lax.rsqrt(jnp.sum(hid * hid, axis=0, keepdims=True) * (1.0 / D) + NORM_EPS)
    xt = hid * inv * (1.0 + w_ref[...])
    xt_ref[...] = xt.astype(jnp.bfloat16)
    x_ref[...] = jnp.transpose(xt).astype(jnp.bfloat16)
    acc[...] = jnp.zeros_like(acc)
    nv = tab_ref.shape[1] // vt
    tb = x_ref.shape[0]

    def step(j, carry):
        cols = pl.ds(pl.multiple_of(j * vt, vt), vt)
        tab = tab_ref[:, cols]
        for i in range(tb // rs):
            rows = pl.ds(i * rs, rs)
            z = jnp.dot(x_ref[rows, :], tab, preferred_element_type=jnp.float32)
            ths = jnp.tanh(z * CAP_INV)
            es = jnp.exp2(ths * CAP_LOG2E)
            tht = jnp.tanh(tea_ref[rows, cols].astype(jnp.float32) * CAP_INV)
            et = jnp.exp2(tht * CAP_LOG2E)
            wt = et * (tht - ths)
            def fold(a):
                r = a[:, 0:128]
                for k in range(1, vt // 128):
                    r = r + a[:, k * 128:(k + 1) * 128]
                return r
            acc[0, rows, :] += fold(es)
            acc[1, rows, :] += fold(et)
            acc[2, rows, :] += fold(wt)
        return carry
    lax.fori_loop(0, nv, step, 0)
    for k in range(3):
        sums = jnp.sum(jnp.transpose(acc[k]), axis=0, keepdims=True)
        for q in range(tb // 128):
            st_ref[pl.ds((k * pl.num_programs(0) + pl.program_id(0)) * (tb // 128) + q, 1), :] = sums[:, q * 128:(q + 1) * 128]


def forward(hid_t, w_col, tab_t, tea, tb=512, vt=2048, rs=128):
    t, v = tea.shape
    return pl.pallas_call(
        functools.partial(stats_kernel, vt, rs),
        grid=(t // tb,),
        out_shape=(jax.ShapeDtypeStruct((t, D), jnp.bfloat16), jax.ShapeDtypeStruct((D, t), jnp.bfloat16), jax.ShapeDtypeStruct((3 * t // 128, 128), jnp.float32)),
        in_specs=[pl.BlockSpec((D, tb), lambda i: (0, i)), pl.BlockSpec((D, 1), lambda i: (0, 0)), pl.BlockSpec((D, v), lambda i: (0, 0), pipeline_mode=pl.Buffered(1)), pl.BlockSpec((tb, v), lambda i: (i, 0))],
        out_specs=(pl.BlockSpec((tb, D), lambda i: (i, 0)), pl.BlockSpec((D, tb), lambda i: (0, i)), pl.BlockSpec((3 * t // 128, 128), lambda i: (0, 0))),
        scratch_shapes=[pltpu.VMEM((3, tb, 128), jnp.float32)],
        compiler_params=pltpu.CompilerParams(vmem_limit_bytes=67043328),
        name='forward',
    )(hid_t, w_col, tab_t, tea)


VBLK = 256
TBLK = 1024
LAG = 2
NPART = 3
PROWS = D // NPART


def backward_kernel(nblk, ntok, tp, dp, x_hbm, xt_hbm, st_ref, mask_ref, w_ref, hid_ref, tab_ref, tea_ref,
                    out_ref, dh_ref, small_ref, land_ref, gath_ref,
                    x_ref, xt_ref, part, near, far, dxt, gbuf, tea_buf, tab_buf, coef_s, coef_t, sbuf, mbuf, slab, load, stage, hbuf, acc_a, acc_b, mloc,
                    blk_sem, send1, recv1, send2, recv2, send3, recv3, store_sem, ssem, srecv, msem, mrecv, rsem, rrecv, gsem, grecv,
                    asem, arecv, bsem, brecv, lsem, hsem, osem, xsem):
    z = lax.axis_index('dp')
    t = lax.axis_index('tp')
    inner = jnp.logical_or(z == 1, z == 2)
    outer = jnp.logical_or(z == 0, z == 3)
    across = 3 - z
    beside = jnp.where(z < 2, 1 - z, 5 - z)
    nch = nblk * NPART
    rows16 = ntok // 128
    slice_cols = ntok // tp

    def remote(src, dst, ssem_, rsem_, **where):
        return pltpu.make_async_remote_copy(src_ref=src, dst_ref=dst, send_sem=ssem_, recv_sem=rsem_, device_id=where, device_id_type=MESH)

    def tea_load(b):
        return pltpu.make_async_copy(tea_ref.at[:, pl.ds(pl.multiple_of(b * VBLK, VBLK), VBLK)], tea_buf.at[b % 2], blk_sem.at[0, b % 2])

    def tab_load(b):
        return pltpu.make_async_copy(tab_ref.at[:, pl.ds(pl.multiple_of(b * VBLK, VBLK), VBLK)], tab_buf.at[b % 2], blk_sem.at[1, b % 2])

    x_load = pltpu.make_async_copy(x_hbm, x_ref, xsem.at[0])
    xt_load = pltpu.make_async_copy(xt_hbm, xt_ref, xsem.at[1])
    tab_load(0).start()
    x_load.start()
    tea_load(0).start()
    xt_load.start()
    hid_load = pltpu.make_async_copy(hid_ref.at[:, pl.ds(pl.multiple_of(t * slice_cols, slice_cols), slice_cols)], hbuf.at[0], hsem)
    hid_load.start()
    mloc[...] = mask_ref[0:8, :] + mask_ref[8:16, :]

    barrier = pltpu.get_barrier_semaphore()
    for i in range(1, tp):
        pl.semaphore_signal(barrier, inc=1, device_id={'tp': lax.rem(t + i, tp)}, device_id_type=MESH)
    for i in range(1, dp):
        pl.semaphore_signal(barrier, inc=1, device_id={'dp': lax.rem(z + i, dp)}, device_id_type=MESH)
    pl.semaphore_wait(barrier, tp + dp - 2)

    for i in range(1, tp):
        remote(st_ref, sbuf.at[t], ssem.at[i], srecv.at[t], tp=lax.rem(t + i, tp)).start()
    for i in range(1, dp):
        remote(mloc, mbuf.at[z], msem.at[i], mrecv.at[z], dp=lax.rem(z + i, dp)).start()
    sbuf[t] = st_ref[...]
    mbuf[z] = mloc[...]
    for i in range(1, tp):
        j = lax.rem(t + i, tp)
        remote(st_ref, sbuf.at[j], ssem.at[i], srecv.at[j], tp=j).wait_recv()
    for i in range(1, dp):
        j = lax.rem(z + i, dp)
        remote(mloc, mbuf.at[j], msem.at[i], mrecv.at[j], dp=j).wait_recv()
    sums = sbuf[0]
    for i in range(1, tp):
        sums = sums + sbuf[i]
    count = mbuf[0]
    for i in range(1, dp):
        count = count + mbuf[i]
    mask_sum = jnp.sum(jnp.sum(count, axis=0, keepdims=True), axis=1, keepdims=True)
    stu_sum, tea_sum, cross = sums[0:rows16], sums[rows16:2 * rows16], sums[2 * rows16:3 * rows16]
    mask = mask_ref[...]
    kl = SOFT_CAP * cross / tea_sum + jnp.log(stu_sum) - jnp.log(tea_sum)
    lrow = jnp.sum(mask * kl, axis=0, keepdims=True)
    weight = mask / mask_sum
    for coef, norm in ((coef_s, stu_sum), (coef_t, tea_sum)):
        ratio = weight / norm
        for r in range(rows16):
            coef[r * 128:(r + 1) * 128, :] = jnp.transpose(jnp.broadcast_to(ratio[r:r + 1, :], (128, 128)))
    dxt[...] = jnp.zeros_like(dxt)

    def fetch(b):
        tea_load(b).wait()
        tab_load(b).wait()

        @pl.when(b + 1 < nblk)
        def _():
            tea_load(b + 1).start()
            tab_load(b + 1).start()

    def tile(b, i):
        slot = b % 2
        rows = pl.ds(i * TBLK, TBLK)
        tab = tab_buf[slot]
        logits = jnp.dot(x_ref[rows, :], tab, preferred_element_type=jnp.float32)
        ths = jnp.tanh(logits * CAP_INV)
        tht = jnp.tanh(tea_buf[slot, rows, :].astype(jnp.float32) * CAP_INV)
        cs, ct = coef_s[rows, :], coef_t[rows, :]
        cs2 = jnp.concatenate([cs, cs], axis=1)
        ct2 = jnp.concatenate([ct, ct], axis=1)
        g = (jnp.exp2(ths * CAP_LOG2E) * cs2 - jnp.exp2(tht * CAP_LOG2E) * ct2) * (1.0 - ths * ths)
        g = g.astype(jnp.bfloat16)
        gbuf[rows, :] = g
        dxt[:, rows] += lax.dot_general(tab, g, (((1,), (1,)), ((), ())), preferred_element_type=jnp.float32)

    def table(b):
        part[pl.ds(b * NPART, NPART)] = jnp.dot(xt_ref[...], gbuf[...], preferred_element_type=jnp.float32).reshape(NPART, PROWS, VBLK)

        @pl.when(outer)
        def _():
            for q in range(NPART):
                c = b * NPART + q
                remote(part.at[c], near.at[c], send1, recv1.at[c], dp=beside).start()

    def place(c):
        return out_ref.at[pl.ds(pl.multiple_of((c % NPART) * PROWS, PROWS), PROWS), pl.ds(pl.multiple_of((c // NPART) * VBLK, VBLK), VBLK)]

    def swap(c):
        return remote(part.at[c], far.at[c], send2, recv2.at[c], dp=across)

    def first(c):
        remote(part.at[c], near.at[c], send1, recv1.at[c], dp=beside).wait_recv()
        part[c] = part[c] + near[c]
        swap(c).start()

    def finish(c):
        swap(c).wait_recv()
        far[c] = far[c] + part[c]
        remote(far.at[c], place(c), send3, recv3, dp=beside).start()
        pltpu.make_async_copy(far.at[c], place(c), store_sem).start()

    def comm(k):
        @pl.when(inner)
        def _():
            for q in range(1):
                c = 1 * k + q
                first(c)

                @pl.when(c >= LAG)
                def _():
                    finish(c - LAG)

    def loop(lo, hi, body):
        def step(k, carry):
            body(k)
            return carry
        lax.fori_loop(lo, hi, step, 0)

    def half(h):
        b = h // 2

        @pl.when(h % 2 == 0)
        def _():
            fetch(b)
            tile(b, 0)

        @pl.when(h % 2 == 1)
        def _():
            tile(b, 1)
            table(b)

    def both(h):
        half(h)

        @pl.when(jnp.logical_and(h >= 2, (h - 2) % 4 != 3))
        def _():
            comm(h - 2 - (h - 2) // 4)
    x_load.wait()
    xt_load.wait()
    loop(0, 2 * nblk, both)

    def cols_of(j):
        return pl.ds(pl.multiple_of(j * slice_cols, slice_cols), slice_cols)
    for i in range(1, tp):
        j = lax.rem(t + i, tp)
        remote(dxt.at[:, cols_of(j)], land_ref.at[t], rsem.at[i], rrecv.at[t], tp=j).start()
    k1 = 2 * nblk - 2 - (2 * nblk - 2) // 4
    k2 = k1 + 13
    loop(k1, k2, comm)
    stage[...] = dxt[:, cols_of(t)]

    def landed(i):
        j = lax.rem(t + i, tp)
        remote(dxt.at[:, cols_of(j)], land_ref.at[j], rsem.at[i], rrecv.at[j], tp=j).wait_recv()
        return pltpu.make_async_copy(land_ref.at[j], load.at[i % 2], lsem.at[i % 2])

    def gather(k):
        i = 2 * (k - k2) + 1
        one, two = landed(i), landed(i + 1)
        one.start()
        two.start()
        comm(k)
        one.wait()
        stage[...] += load[1]
        two.wait()
        stage[...] += load[0]
    k3 = k2 + tp // 2
    loop(k2, k3 - 1, gather)
    last = landed(tp - 1)
    last.start()
    comm(k3 - 1)
    last.wait()
    stage[...] += load[1]
    hid_load.wait()
    hid = hbuf[0].astype(jnp.float32)
    inv = lax.rsqrt(jnp.sum(hid * hid, axis=0, keepdims=True) * (1.0 / D) + NORM_EPS)
    normed = hid * inv
    dx = stage[...]
    gain = dx * normed
    gain = sum((gain[:, q * 128:(q + 1) * 128] for q in range(1, slice_cols // 128)), gain[:, 0:128])
    load[0, :, 0:128] = gain
    slab[...] = jnp.zeros_like(slab)
    for q in range(5):
        lo, hi = q * 128, min(D, q * 128 + 128)
        sq = load[0, lo:hi, 0:128]
        if hi - lo < 128:
            sq = jnp.concatenate([sq, jnp.zeros((128 - (hi - lo), 128), jnp.float32)], axis=0)
        slab[0:1, lo:lo + 128] = jnp.sum(jnp.transpose(sq), axis=0, keepdims=True)
    slab[1:2, 0:128] = lrow
    grad_n = dx * (1.0 + w_ref[...])
    stage[...] = inv * (grad_n - normed * (jnp.sum(grad_n * normed, axis=0, keepdims=True) * (1.0 / D)))
    for i in range(1, tp):
        j = lax.rem(t + i, tp)
        remote(slab, acc_a.at[t], asem.at[i], arecv.at[t], tp=j).start()
        remote(stage, gath_ref.at[t], gsem.at[i], grecv.at[t], tp=j).start()
    acc_a[t] = slab[...]

    def emit(j, src, slot):
        hbuf[slot] = src.astype(jnp.bfloat16)
        return pltpu.make_async_copy(hbuf.at[slot], dh_ref.at[:, cols_of(j)], osem.at[slot])
    own = emit(t, stage[...], 1)
    own.start()
    nstep = nch // 1
    k4 = nstep - tp // 2 - 1
    loop(k3, k4, comm)
    own.wait()
    for i in range(1, tp):
        j = lax.rem(t + i, tp)
        remote(slab, acc_a.at[j], asem.at[i], arecv.at[j], tp=j).wait_recv()
    tot = acc_a[0]
    for i in range(1, tp):
        tot = tot + acc_a[i]
    hbuf_row = lax.broadcasted_iota(jnp.int32, tot.shape, 0) == 0
    acc_b[z] = jnp.where(hbuf_row, tot, slab[...])
    for i in range(1, dp):
        j = lax.rem(z + i, dp)
        remote(acc_b.at[z], acc_b.at[z], bsem.at[i], brecv.at[z], dp=j).start()

    def spread_load(i):
        j = lax.rem(t + i, tp)
        remote(stage, gath_ref.at[j], gsem.at[i], grecv.at[j], tp=j).wait_recv()
        return pltpu.make_async_copy(gath_ref.at[j], load.at[i % 2], lsem.at[i % 2])

    def spread(k):
        i = 2 * (k - k4) + 1
        one, two = spread_load(i), spread_load(i + 1)
        one.start()
        two.start()
        comm(k)
        one.wait()
        out1 = emit(lax.rem(t + i, tp), load[1], 1)
        out1.start()
        two.wait()
        out2 = emit(lax.rem(t + i + 1, tp), load[0], 0)
        out2.start()
        out1.wait()
        out2.wait()
    loop(k4, k4 + tp // 2 - 1, spread)
    tail = spread_load(tp - 1)
    tail.start()
    comm(k4 + tp // 2 - 1)
    tail.wait()
    final = emit(lax.rem(t + tp - 1, tp), load[1], 1)
    final.start()
    loop(k4 + tp // 2, nstep, comm)
    final.wait()

    for i in range(1, dp):
        j = lax.rem(z + i, dp)
        remote(acc_b.at[j], acc_b.at[j], bsem.at[i], brecv.at[j], dp=j).wait_recv()
    tot = acc_b[0]
    for i in range(1, dp):
        tot = tot + acc_b[i]
    loss = jnp.sum(tot[1:2, 0:128], axis=1, keepdims=True) / mask_sum
    row = lax.broadcasted_iota(jnp.int32, tot.shape, 0)
    small_ref[...] = jnp.where(row == 1, loss, tot)

    @pl.when(inner)
    def _():
        for c in range(nch - LAG, nch):
            finish(c)
        remote(part, far, send2, recv2.at[0], dp=across).wait_send()
        remote(far, far, send3, recv3, dp=beside).wait_send()
        pltpu.make_async_copy(out_ref, out_ref, store_sem).wait()

    @pl.when(outer)
    def _():
        remote(part, near, send1, recv1.at[0], dp=beside).wait_send()
        remote(out_ref, out_ref, send3, recv3, dp=beside).wait_recv()

    for i in range(1, tp):
        j = lax.rem(t + i, tp)
        remote(st_ref, sbuf.at[t], ssem.at[i], srecv.at[t], tp=j).wait_send()
        remote(dxt.at[:, cols_of(j)], land_ref.at[t], rsem.at[i], rrecv.at[t], tp=j).wait_send()
        remote(slab, acc_a.at[t], asem.at[i], arecv.at[t], tp=j).wait_send()
        remote(stage, gath_ref.at[t], gsem.at[i], grecv.at[t], tp=j).wait_send()
    for i in range(1, dp):
        j = lax.rem(z + i, dp)
        remote(mloc, mbuf.at[z], msem.at[i], mrecv.at[z], dp=j).wait_send()
        remote(acc_b.at[z], acc_b.at[z], bsem.at[i], brecv.at[z], dp=j).wait_send()


def backward(mesh, x, xt, stats, mask, w_col, hid_t, tab_t, tea):
    tp, dp = mesh.shape['tp'], mesh.shape['dp']
    ntok, vocab = tea.shape
    nblk = vocab // VBLK
    nch = nblk * NPART
    sl = ntok // tp
    f32, bf16 = jnp.float32, jnp.bfloat16
    dma = pltpu.SemaphoreType.DMA
    vmem = pl.BlockSpec(memory_space=pltpu.VMEM)
    hbm = pl.BlockSpec(memory_space=pl.ANY)
    chunks = pltpu.VMEM((nch, PROWS, VBLK), f32)
    out, dh, small, _, _ = pl.pallas_call(
        functools.partial(backward_kernel, nblk, ntok, tp, dp),
        out_shape=(jax.ShapeDtypeStruct((D, vocab), f32), jax.ShapeDtypeStruct((D, ntok), bf16), jax.ShapeDtypeStruct((8, 640), f32),
                   jax.ShapeDtypeStruct((tp, D, sl), f32), jax.ShapeDtypeStruct((tp, D, sl), f32)),
        in_specs=[hbm, hbm, vmem, vmem, vmem, hbm, hbm, hbm],
        out_specs=(hbm, hbm, vmem, hbm, hbm),
        scratch_shapes=[
            pltpu.VMEM((ntok, D), bf16), pltpu.VMEM((D, ntok), bf16), chunks, chunks, chunks, pltpu.VMEM((D, ntok), f32), pltpu.VMEM((ntok, VBLK), bf16), pltpu.VMEM((2, ntok, VBLK), bf16),
            pltpu.VMEM((2, D, VBLK), bf16), pltpu.VMEM((ntok, 128), f32), pltpu.VMEM((ntok, 128), f32), pltpu.VMEM((tp, 3 * ntok // 128, 128), f32),
            pltpu.VMEM((dp, 8, 128), f32), pltpu.VMEM((8, 640), f32), pltpu.VMEM((2, D, sl), f32), pltpu.VMEM((D, sl), f32), pltpu.VMEM((2, D, sl), bf16),
            pltpu.VMEM((tp, 8, 640), f32), pltpu.VMEM((dp, 8, 640), f32), pltpu.VMEM((8, 128), f32),
            dma((2, 2)), dma, dma((nch,)), dma, dma((nch,)), dma, dma, dma, dma((tp,)), dma((tp,)), dma((dp,)), dma((dp,)),
            dma((tp,)), dma((tp,)), dma((tp,)), dma((tp,)), dma((tp,)), dma((tp,)), dma((dp,)), dma((dp,)), dma((2,)), dma, dma((2,)), dma((2,))],
        compiler_params=pltpu.CompilerParams(collective_id=0, has_side_effects=True, vmem_limit_bytes=67043328),
        name='backward',
    )(x, xt, stats, mask, w_col, hid_t, tab_t, tea)
    return out, dh, small


def emit_kernel(table_ref, dh_ref, small_ref, table_out, dh_out, gain_out, loss_out):
    table_out[...] = table_ref[...]
    dh_out[...] = dh_ref[...]
    gain_out[...] = small_ref[0:1, 0:D]
    loss_out[...] = small_ref[1:2, 0:1]


def emit(table, dh, small, rows=48):
    vocab, ntok = table.shape[1], dh.shape[1]
    band = pl.BlockSpec((rows, vocab), lambda i: (i, 0))
    hid = pl.BlockSpec((rows, ntok), lambda i: (i, 0))

    def whole(*shape):
        return pl.BlockSpec(shape, lambda i: (0, 0))
    return pl.pallas_call(
        emit_kernel,
        grid=(D // rows,),
        out_shape=(jax.ShapeDtypeStruct(table.shape, table.dtype), jax.ShapeDtypeStruct(dh.shape, dh.dtype), jax.ShapeDtypeStruct((1, D), jnp.float32), jax.ShapeDtypeStruct((1, 1), jnp.float32)),
        in_specs=[band, hid, whole(*small.shape)],
        out_specs=(band, hid, whole(1, D), whole(1, 1)),
        name='emit',
    )(table, dh, small)


def solution(mesh):
    def local_step(hid_rows, w_final, tab_rows, tea_rows, mask_rows):
        w_col = w_final[:, None]
        hid_t, tab_t = hid_rows.T, tab_rows.T
        x, xt, stats = forward(hid_t, w_col, tab_t, tea_rows)
        mask = mask_rows.reshape(-1, 128)
        grad_table, grad_hid, small = backward(mesh, x, xt, stats, mask, w_col, hid_t, tab_t, tea_rows)
        grad_table, grad_hid, gain, loss = emit(grad_table, grad_hid, small)
        return loss[0, 0], grad_hid.T, gain[0], grad_table.T

    return jax.shard_map(local_step, mesh=mesh, in_specs=(P('dp', None), P(None), P('tp', None), P('dp', 'tp'), P('dp')), out_specs=(P(), P('dp', None), P(None), P('tp', None)), check_vma=False)
```

```python
import functools
import jax, jax.numpy as jnp
from jax import lax
from jax.experimental import pallas as pl
from jax.experimental.pallas import tpu as pltpu

from jax.sharding import PartitionSpec as P

MESH = pl.DeviceIdType.MESH
SOFT_CAP = 30.0
CAP_INV = 1.0 / 30.0
CAP_LOG2E = 30.0 * 1.4426950408889634
NORM_EPS = 1e-6
D = 576

def stats_kernel(vt, rs, hid_ref, w_ref, tab_ref, tea_ref, x_ref, xt_ref, st_ref, acc):
    hid = hid_ref[...].astype(jnp.float32)
    inv = lax.rsqrt(jnp.sum(hid * hid, axis=0, keepdims=True) * (1.0 / D) + NORM_EPS)
    xt = hid * inv * (1.0 + w_ref[...])
    xt_ref[...] = xt.astype(jnp.bfloat16)
    x_ref[...] = jnp.transpose(xt).astype(jnp.bfloat16)
    acc[...] = jnp.zeros_like(acc)
    nv = tab_ref.shape[1] // vt
    tb = x_ref.shape[0]

    def step(j, carry):
        cols = pl.ds(pl.multiple_of(j * vt, vt), vt)
        tab = tab_ref[:, cols]
        for i in range(tb // rs):
            rows = pl.ds(i * rs, rs)
            z = jnp.dot(x_ref[rows, :], tab, preferred_element_type=jnp.float32)
            ths = jnp.tanh(z * CAP_INV)
            es = jnp.exp2(ths * CAP_LOG2E)
            tht = jnp.tanh(tea_ref[rows, cols].astype(jnp.float32) * CAP_INV)
            et = jnp.exp2(tht * CAP_LOG2E)
            wt = et * (tht - ths)
            def fold(a):
                r = a[:, 0:128]
                for k in range(1, vt // 128):
                    r = r + a[:, k * 128:(k + 1) * 128]
                return r
            acc[0, rows, :] += fold(es)
            acc[1, rows, :] += fold(et)
            acc[2, rows, :] += fold(wt)
        return carry
    lax.fori_loop(0, nv, step, 0)
    for k in range(3):
        sums = jnp.sum(jnp.transpose(acc[k]), axis=0, keepdims=True)
        for q in range(tb // 128):
            st_ref[pl.ds((k * pl.num_programs(0) + pl.program_id(0)) * (tb // 128) + q, 1), :] = sums[:, q * 128:(q + 1) * 128]


def forward(hid_t, w_col, tab_t, tea, tb=512, vt=2048, rs=128):
    t, v = tea.shape
    return pl.pallas_call(
        functools.partial(stats_kernel, vt, rs),
        grid=(t // tb,),
        out_shape=(jax.ShapeDtypeStruct((t, D), jnp.bfloat16), jax.ShapeDtypeStruct((D, t), jnp.bfloat16), jax.ShapeDtypeStruct((3 * t // 128, 128), jnp.float32)),
        in_specs=[pl.BlockSpec((D, tb), lambda i: (0, i)), pl.BlockSpec((D, 1), lambda i: (0, 0)), pl.BlockSpec((D, v), lambda i: (0, 0), pipeline_mode=pl.Buffered(1)), pl.BlockSpec((tb, v), lambda i: (i, 0))],
        out_specs=(pl.BlockSpec((tb, D), lambda i: (i, 0)), pl.BlockSpec((D, tb), lambda i: (0, i)), pl.BlockSpec((3 * t // 128, 128), lambda i: (0, 0))),
        scratch_shapes=[pltpu.VMEM((3, tb, 128), jnp.float32)],
        compiler_params=pltpu.CompilerParams(vmem_limit_bytes=67043328),
        name='forward',
    )(hid_t, w_col, tab_t, tea)


VBLK = 256
TBLK = 1024
LAG = 2
NPART = 3
PROWS = D // NPART


def backward_kernel(nblk, ntok, tp, dp, x_hbm, xt_hbm, st_ref, mask_ref, w_ref, hid_ref, tab_ref, tea_ref,
                    out_ref, dh_ref, small_ref, land_ref, gath_ref,
                    x_ref, xt_ref, part, near, far, dxt, gbuf, tea_buf, tab_buf, coef_s, coef_t, sbuf, mbuf, slab, load, stage, hbuf, acc_a, acc_b, mloc,
                    blk_sem, send1, recv1, send2, recv2, send3, recv3, store_sem, ssem, srecv, msem, mrecv, rsem, rrecv, gsem, grecv,
                    asem, arecv, bsem, brecv, lsem, hsem, osem, xsem):
    z = lax.axis_index('dp')
    t = lax.axis_index('tp')
    inner = jnp.logical_or(z == 1, z == 2)
    outer = jnp.logical_or(z == 0, z == 3)
    across = 3 - z
    beside = jnp.where(z < 2, 1 - z, 5 - z)
    nch = nblk * NPART
    rows16 = ntok // 128
    slice_cols = ntok // tp

    def remote(src, dst, ssem_, rsem_, **where):
        return pltpu.make_async_remote_copy(src_ref=src, dst_ref=dst, send_sem=ssem_, recv_sem=rsem_, device_id=where, device_id_type=MESH)

    def tea_load(b):
        return pltpu.make_async_copy(tea_ref.at[:, pl.ds(pl.multiple_of(b * VBLK, VBLK), VBLK)], tea_buf.at[b % 2], blk_sem.at[0, b % 2])

    def tab_load(b):
        return pltpu.make_async_copy(tab_ref.at[:, pl.ds(pl.multiple_of(b * VBLK, VBLK), VBLK)], tab_buf.at[b % 2], blk_sem.at[1, b % 2])

    x_load = pltpu.make_async_copy(x_hbm, x_ref, xsem.at[0])
    xt_load = pltpu.make_async_copy(xt_hbm, xt_ref, xsem.at[1])
    tab_load(0).start()
    x_load.start()
    tea_load(0).start()
    xt_load.start()
    hid_load = pltpu.make_async_copy(hid_ref.at[:, pl.ds(pl.multiple_of(t * slice_cols, slice_cols), slice_cols)], hbuf.at[0], hsem)
    hid_load.start()
    mloc[...] = mask_ref[0:8, :] + mask_ref[8:16, :]

    barrier = pltpu.get_barrier_semaphore()
    for i in range(1, tp):
        pl.semaphore_signal(barrier, inc=1, device_id={'tp': lax.rem(t + i, tp)}, device_id_type=MESH)
    for i in range(1, dp):
        pl.semaphore_signal(barrier, inc=1, device_id={'dp': lax.rem(z + i, dp)}, device_id_type=MESH)
    pl.semaphore_wait(barrier, tp + dp - 2)

    for i in range(1, tp):
        remote(st_ref, sbuf.at[t], ssem.at[i], srecv.at[t], tp=lax.rem(t + i, tp)).start()
    for i in range(1, dp):
        remote(mloc, mbuf.at[z], msem.at[i], mrecv.at[z], dp=lax.rem(z + i, dp)).start()
    sbuf[t] = st_ref[...]
    mbuf[z] = mloc[...]
    for i in range(1, tp):
        j = lax.rem(t + i, tp)
        remote(st_ref, sbuf.at[j], ssem.at[i], srecv.at[j], tp=j).wait_recv()
    for i in range(1, dp):
        j = lax.rem(z + i, dp)
        remote(mloc, mbuf.at[j], msem.at[i], mrecv.at[j], dp=j).wait_recv()
    sums = sbuf[0]
    for i in range(1, tp):
        sums = sums + sbuf[i]
    count = mbuf[0]
    for i in range(1, dp):
        count = count + mbuf[i]
    mask_sum = jnp.sum(jnp.sum(count, axis=0, keepdims=True), axis=1, keepdims=True)
    stu_sum, tea_sum, cross = sums[0:rows16], sums[rows16:2 * rows16], sums[2 * rows16:3 * rows16]
    mask = mask_ref[...]
    kl = SOFT_CAP * cross / tea_sum + jnp.log(stu_sum) - jnp.log(tea_sum)
    lrow = jnp.sum(mask * kl, axis=0, keepdims=True)
    weight = mask / mask_sum
    for coef, norm in ((coef_s, stu_sum), (coef_t, tea_sum)):
        ratio = weight / norm
        for r in range(rows16):
            coef[r * 128:(r + 1) * 128, :] = jnp.transpose(jnp.broadcast_to(ratio[r:r + 1, :], (128, 128)))
    dxt[...] = jnp.zeros_like(dxt)

    def fetch(b):
        tea_load(b).wait()
        tab_load(b).wait()

        @pl.when(b + 1 < nblk)
        def _():
            tea_load(b + 1).start()
            tab_load(b + 1).start()

    def tile(b, i):
        slot = b % 2
        rows = pl.ds(i * TBLK, TBLK)
        tab = tab_buf[slot]
        logits = jnp.dot(x_ref[rows, :], tab, preferred_element_type=jnp.float32)
        ths = jnp.tanh(logits * CAP_INV)
        tht = jnp.tanh(tea_buf[slot, rows, :].astype(jnp.float32) * CAP_INV)
        cs, ct = coef_s[rows, :], coef_t[rows, :]
        cs2 = jnp.concatenate([cs, cs], axis=1)
        ct2 = jnp.concatenate([ct, ct], axis=1)
        g = (jnp.exp2(ths * CAP_LOG2E) * cs2 - jnp.exp2(tht * CAP_LOG2E) * ct2) * (1.0 - ths * ths)
        g = g.astype(jnp.bfloat16)
        gbuf[rows, :] = g
        dxt[:, rows] += lax.dot_general(tab, g, (((1,), (1,)), ((), ())), preferred_element_type=jnp.float32)

    def table(b):
        part[pl.ds(b * NPART, NPART)] = jnp.dot(xt_ref[...], gbuf[...], preferred_element_type=jnp.float32).reshape(NPART, PROWS, VBLK)

        @pl.when(outer)
        def _():
            for q in range(NPART):
                c = b * NPART + q
                remote(part.at[c], near.at[c], send1, recv1.at[c], dp=beside).start()

    def place(c):
        return out_ref.at[pl.ds(pl.multiple_of((c % NPART) * PROWS, PROWS), PROWS), pl.ds(pl.multiple_of((c // NPART) * VBLK, VBLK), VBLK)]

    def swap(c):
        return remote(part.at[c], far.at[c], send2, recv2.at[c], dp=across)

    def first(c):
        remote(part.at[c], near.at[c], send1, recv1.at[c], dp=beside).wait_recv()
        part[c] = part[c] + near[c]
        swap(c).start()

    def finish(c):
        swap(c).wait_recv()
        far[c] = far[c] + part[c]
        remote(far.at[c], place(c), send3, recv3, dp=beside).start()
        pltpu.make_async_copy(far.at[c], place(c), store_sem).start()

    def comm(k):
        @pl.when(inner)
        def _():
            for q in range(1):
                c = 1 * k + q
                first(c)

                @pl.when(c >= LAG)
                def _():
                    finish(c - LAG)

    def loop(lo, hi, body):
        def step(k, carry):
            body(k)
            return carry
        lax.fori_loop(lo, hi, step, 0)

    def half(h):
        b = h // 2

        @pl.when(h % 2 == 0)
        def _():
            fetch(b)
            tile(b, 0)

        @pl.when(h % 2 == 1)
        def _():
            tile(b, 1)
            table(b)

    def both(h):
        half(h)

        @pl.when(jnp.logical_and(h >= 2, (h - 2) % 4 != 3))
        def _():
            comm(h - 2 - (h - 2) // 4)
    x_load.wait()
    xt_load.wait()
    loop(0, 2 * nblk, both)

    def cols_of(j):
        return pl.ds(pl.multiple_of(j * slice_cols, slice_cols), slice_cols)
    for i in range(1, tp):
        j = lax.rem(t + i, tp)
        remote(dxt.at[:, cols_of(j)], land_ref.at[t], rsem.at[i], rrecv.at[t], tp=j).start()
    k1 = 2 * nblk - 2 - (2 * nblk - 2) // 4
    k2 = k1 + 13
    loop(k1, k2, comm)
    stage[...] = dxt[:, cols_of(t)]

    def landed(i):
        j = lax.rem(t + i, tp)
        remote(dxt.at[:, cols_of(j)], land_ref.at[j], rsem.at[i], rrecv.at[j], tp=j).wait_recv()
        return pltpu.make_async_copy(land_ref.at[j], load.at[i % 2], lsem.at[i % 2])

    def gather(k):
        i = 2 * (k - k2) + 1
        one, two = landed(i), landed(i + 1)
        one.start()
        two.start()
        comm(k)
        one.wait()
        stage[...] += load[1]
        two.wait()
        stage[...] += load[0]
    k3 = k2 + tp // 2
    loop(k2, k3 - 1, gather)
    last = landed(tp - 1)
    last.start()
    comm(k3 - 1)
    last.wait()
    stage[...] += load[1]
    hid_load.wait()
    hid = hbuf[0].astype(jnp.float32)
    inv = lax.rsqrt(jnp.sum(hid * hid, axis=0, keepdims=True) * (1.0 / D) + NORM_EPS)
    normed = hid * inv
    dx = stage[...]
    gain = dx * normed
    gain = sum((gain[:, q * 128:(q + 1) * 128] for q in range(1, slice_cols // 128)), gain[:, 0:128])
    load[0, :, 0:128] = gain
    slab[...] = jnp.zeros_like(slab)
    for q in range(5):
        lo, hi = q * 128, min(D, q * 128 + 128)
        sq = load[0, lo:hi, 0:128]
        if hi - lo < 128:
            sq = jnp.concatenate([sq, jnp.zeros((128 - (hi - lo), 128), jnp.float32)], axis=0)
        slab[0:1, lo:lo + 128] = jnp.sum(jnp.transpose(sq), axis=0, keepdims=True)
    slab[1:2, 0:128] = lrow
    grad_n = dx * (1.0 + w_ref[...])
    stage[...] = inv * (grad_n - normed * (jnp.sum(grad_n * normed, axis=0, keepdims=True) * (1.0 / D)))
    for i in range(1, tp):
        j = lax.rem(t + i, tp)
        remote(slab, acc_a.at[t], asem.at[i], arecv.at[t], tp=j).start()
        remote(stage, gath_ref.at[t], gsem.at[i], grecv.at[t], tp=j).start()
    acc_a[t] = slab[...]

    def emit(j, src, slot):
        hbuf[slot] = src.astype(jnp.bfloat16)
        return pltpu.make_async_copy(hbuf.at[slot], dh_ref.at[:, cols_of(j)], osem.at[slot])
    own = emit(t, stage[...], 1)
    own.start()
    nstep = nch // 1
    k4 = nstep - tp // 2 - 1
    loop(k3, k4, comm)
    own.wait()
    for i in range(1, tp):
        j = lax.rem(t + i, tp)
        remote(slab, acc_a.at[j], asem.at[i], arecv.at[j], tp=j).wait_recv()
    tot = acc_a[0]
    for i in range(1, tp):
        tot = tot + acc_a[i]
    hbuf_row = lax.broadcasted_iota(jnp.int32, tot.shape, 0) == 0
    acc_b[z] = jnp.where(hbuf_row, tot, slab[...])
    for i in range(1, dp):
        j = lax.rem(z + i, dp)
        remote(acc_b.at[z], acc_b.at[z], bsem.at[i], brecv.at[z], dp=j).start()

    def spread_load(i):
        j = lax.rem(t + i, tp)
        remote(stage, gath_ref.at[j], gsem.at[i], grecv.at[j], tp=j).wait_recv()
        return pltpu.make_async_copy(gath_ref.at[j], load.at[i % 2], lsem.at[i % 2])

    def spread(k):
        i = 2 * (k - k4) + 1
        one, two = spread_load(i), spread_load(i + 1)
        one.start()
        two.start()
        comm(k)
        one.wait()
        out1 = emit(lax.rem(t + i, tp), load[1], 1)
        out1.start()
        two.wait()
        out2 = emit(lax.rem(t + i + 1, tp), load[0], 0)
        out2.start()
        out1.wait()
        out2.wait()
    loop(k4, k4 + tp // 2 - 1, spread)
    tail = spread_load(tp - 1)
    tail.start()
    comm(k4 + tp // 2 - 1)
    tail.wait()
    final = emit(lax.rem(t + tp - 1, tp), load[1], 1)
    final.start()
    loop(k4 + tp // 2, nstep, comm)
    final.wait()

    for i in range(1, dp):
        j = lax.rem(z + i, dp)
        remote(acc_b.at[j], acc_b.at[j], bsem.at[i], brecv.at[j], dp=j).wait_recv()
    tot = acc_b[0]
    for i in range(1, dp):
        tot = tot + acc_b[i]
    loss = jnp.sum(tot[1:2, 0:128], axis=1, keepdims=True) / mask_sum
    row = lax.broadcasted_iota(jnp.int32, tot.shape, 0)
    small_ref[...] = jnp.where(row == 1, loss, tot)

    @pl.when(inner)
    def _():
        for c in range(nch - LAG, nch):
            finish(c)
        remote(part, far, send2, recv2.at[0], dp=across).wait_send()
        remote(far, far, send3, recv3, dp=beside).wait_send()
        pltpu.make_async_copy(out_ref, out_ref, store_sem).wait()

    @pl.when(outer)
    def _():
        remote(part, near, send1, recv1.at[0], dp=beside).wait_send()
        remote(out_ref, out_ref, send3, recv3, dp=beside).wait_recv()

    for i in range(1, tp):
        j = lax.rem(t + i, tp)
        remote(st_ref, sbuf.at[t], ssem.at[i], srecv.at[t], tp=j).wait_send()
        remote(dxt.at[:, cols_of(j)], land_ref.at[t], rsem.at[i], rrecv.at[t], tp=j).wait_send()
        remote(slab, acc_a.at[t], asem.at[i], arecv.at[t], tp=j).wait_send()
        remote(stage, gath_ref.at[t], gsem.at[i], grecv.at[t], tp=j).wait_send()
    for i in range(1, dp):
        j = lax.rem(z + i, dp)
        remote(mloc, mbuf.at[z], msem.at[i], mrecv.at[z], dp=j).wait_send()
        remote(acc_b.at[z], acc_b.at[z], bsem.at[i], brecv.at[z], dp=j).wait_send()


def backward(mesh, x, xt, stats, mask, w_col, hid_t, tab_t, tea):
    tp, dp = mesh.shape['tp'], mesh.shape['dp']
    ntok, vocab = tea.shape
    nblk = vocab // VBLK
    nch = nblk * NPART
    sl = ntok // tp
    f32, bf16 = jnp.float32, jnp.bfloat16
    dma = pltpu.SemaphoreType.DMA
    vmem = pl.BlockSpec(memory_space=pltpu.VMEM)
    hbm = pl.BlockSpec(memory_space=pl.ANY)
    chunks = pltpu.VMEM((nch, PROWS, VBLK), f32)
    out, dh, small, _, _ = pl.pallas_call(
        functools.partial(backward_kernel, nblk, ntok, tp, dp),
        out_shape=(jax.ShapeDtypeStruct((D, vocab), f32), jax.ShapeDtypeStruct((D, ntok), bf16), jax.ShapeDtypeStruct((8, 640), f32),
                   jax.ShapeDtypeStruct((tp, D, sl), f32), jax.ShapeDtypeStruct((tp, D, sl), f32)),
        in_specs=[hbm, hbm, vmem, vmem, vmem, hbm, hbm, hbm],
        out_specs=(hbm, hbm, vmem, hbm, hbm),
        scratch_shapes=[
            pltpu.VMEM((ntok, D), bf16), pltpu.VMEM((D, ntok), bf16), chunks, chunks, chunks, pltpu.VMEM((D, ntok), f32), pltpu.VMEM((ntok, VBLK), bf16), pltpu.VMEM((2, ntok, VBLK), bf16),
            pltpu.VMEM((2, D, VBLK), bf16), pltpu.VMEM((ntok, 128), f32), pltpu.VMEM((ntok, 128), f32), pltpu.VMEM((tp, 3 * ntok // 128, 128), f32),
            pltpu.VMEM((dp, 8, 128), f32), pltpu.VMEM((8, 640), f32), pltpu.VMEM((2, D, sl), f32), pltpu.VMEM((D, sl), f32), pltpu.VMEM((2, D, sl), bf16),
            pltpu.VMEM((tp, 8, 640), f32), pltpu.VMEM((dp, 8, 640), f32), pltpu.VMEM((8, 128), f32),
            dma((2, 2)), dma, dma((nch,)), dma, dma((nch,)), dma, dma, dma, dma((tp,)), dma((tp,)), dma((dp,)), dma((dp,)),
            dma((tp,)), dma((tp,)), dma((tp,)), dma((tp,)), dma((tp,)), dma((tp,)), dma((dp,)), dma((dp,)), dma((2,)), dma, dma((2,)), dma((2,))],
        compiler_params=pltpu.CompilerParams(collective_id=0, has_side_effects=True, vmem_limit_bytes=67043328),
        name='backward',
    )(x, xt, stats, mask, w_col, hid_t, tab_t, tea)
    return out, dh, small


def emit_kernel(table_ref, dh_ref, small_ref, table_out, dh_out, gain_out, loss_out):
    table_out[...] = table_ref[...]
    dh_out[...] = dh_ref[...]
    gain_out[...] = small_ref[0, 0:D]
    loss_out[...] = small_ref[1:2, 0:1]


def emit(table, dh, small, rows=48):
    vocab, ntok = table.shape[1], dh.shape[1]
    band = pl.BlockSpec((rows, vocab), lambda i: (i, 0))
    hid = pl.BlockSpec((rows, ntok), lambda i: (i, 0))

    def whole(*shape):
        return pl.BlockSpec(shape, lambda i: (0, 0))
    return pl.pallas_call(
        emit_kernel,
        grid=(D // rows,),
        out_shape=(jax.ShapeDtypeStruct(table.shape, table.dtype), jax.ShapeDtypeStruct(dh.shape, dh.dtype), jax.ShapeDtypeStruct((D,), jnp.float32), jax.ShapeDtypeStruct((1, 1), jnp.float32)),
        in_specs=[band, hid, whole(*small.shape)],
        out_specs=(band, hid, pl.BlockSpec((D,), lambda i: (0,)), whole(1, 1)),
        name='emit',
    )(table, dh, small)


def solution(mesh):
    def local_step(hid_rows, w_final, tab_rows, tea_rows, mask_rows):
        w_col = w_final[:, None]
        hid_t, tab_t = hid_rows.T, tab_rows.T
        x, xt, stats = forward(hid_t, w_col, tab_t, tea_rows)
        mask = mask_rows.reshape(-1, 128)
        grad_table, grad_hid, small = backward(mesh, x, xt, stats, mask, w_col, hid_t, tab_t, tea_rows)
        grad_table, grad_hid, gain, loss = emit(grad_table, grad_hid, small)
        return loss.reshape(()), grad_hid.T, gain, grad_table.T

    return jax.shard_map(local_step, mesh=mesh, in_specs=(P('dp', None), P(None), P('tp', None), P('dp', 'tp'), P('dp')), out_specs=(P(), P('dp', None), P(None), P('tp', None)), check_vma=False)
```
